32 devices in a mesh: dp: 4 (over x, core), rows: 8 (over z, y).
Axes of the slice: x: 2, y: 2, z: 4, core: 2. Of those that a mesh axis runs over, the one named last changes fastest.
Arguments:
- grads: bfloat16 [2, 4096, 14336], P(None, 'rows', 'dp'), may hold values from -64 to 64
- basis: bfloat16 [2, 4096, 512], P(None, 'rows'), may hold values from -0.09375 to 0.09375
- moment1: float32 [2, 512, 14336], P(None, 'rows', 'dp'), may hold values from -0.3 to 0.3
- moment2: float32 [2, 512, 14336], P(None, 'rows', 'dp'), may hold values from 0.001 to 0.03
- weights: bfloat16 [2, 4096, 14336], P(None, 'rows', 'dp'), may hold values from -0.09375 to 0.09375
Outputs:
- new_weights: bfloat16 [2, 4096, 14336], P(None, 'rows')
- new_moment1: float32 [2, 512, 14336], P(None, 'rows', 'dp')
- new_moment2: float32 [2, 512, 14336], P(None, 'rows', 'dp')
The draws below stay inside these ranges and needn't reach their ends.
All inputs are finite; a program needn't handle non-finite values.
Results may differ from the reference program's by a relative error of at most 0.00115.
The reference program's roundings to bfloat16 on the way count: a program that leaves them out, or rounds other values in their place, can miss the bound.
Values may be sent and summed in bfloat16 or wider, within the bound.
A program may use at most 128 MiB of HBM per device.

```python
import math
import jax
import jax.numpy as jnp

D = 4096
FF = 14336
RANK = 512
MATS = 2
STEP = 10


def draw_grads(key, part):
    key_rows = jax.random.fold_in(key, 11)
    key_cols = jax.random.fold_in(key, 12)
    primary_key = jax.random.fold_in(key, 13)
    row_scale = jnp.repeat(jnp.exp(jax.random.uniform(key_rows, (MATS, D // 32, 1), jnp.float32, -0.7, 0.7)), 32, axis=1)
    col_scale = jnp.repeat(jnp.exp(jax.random.uniform(key_cols, (MATS, 1, FF // 128), jnp.float32, -0.7, 0.7)), 128, axis=2)
    values = 8.0 * jax.random.normal(primary_key, (MATS, D, FF), jnp.float32) * row_scale * col_scale
    return jnp.clip(values, -64.0, 64.0).astype(jnp.bfloat16)


def block_scale(own_key, shape, cuts, low, high):
    factor_of, own = 1.0, jax.random.fold_in(own_key, 6)
    for dim, parts in cuts:
        heights = jnp.exp(jax.random.uniform(jax.random.fold_in(own, dim), (parts,), jnp.float32, low / len(cuts), high / len(cuts)))
        factor_of = factor_of * jnp.repeat(heights, shape[dim] // parts).reshape([-1 if axis == dim else 1 for axis in range(len(shape))])
    return factor_of


def scatter_about(own_key, dims, deviation, most, cuts=(), held_as=jnp.bfloat16):
    entries = deviation * jax.random.normal(own_key, dims, jnp.float32)
    if cuts:
        entries = entries * block_scale(own_key, dims, cuts, -0.22, 0.18)
    return jnp.clip(entries, -most, most).astype(held_as)


def setup_inputs(seed: int = 0) -> dict:
    keys = jax.random.split(jax.random.key(seed), 6)
    grads = draw_grads(jax.random.fold_in(keys[5], 71), 0)
    basis = scatter_about(keys[1], (MATS, D, RANK), D ** -0.5, 0.09375, ((1, 8),))
    moment1 = scatter_about(keys[2], (MATS, RANK, FF), 0.05, 0.3, ((1, 8), (2, 4)), jnp.float32)
    moment2 = jnp.clip(jnp.exp(math.log(0.03) - 3.4011973 * jax.random.uniform(keys[3], (MATS, RANK, FF), jnp.float32) ** block_scale(keys[3], (MATS, RANK, FF), ((1, 8), (2, 4)), -0.2, 0.2)), 0.001, 0.03)
    weights = scatter_about(keys[4], (MATS, D, FF), D ** -0.5, 0.09375, ((1, 8), (2, 4)))
    return dict(grads=grads, basis=basis, moment1=moment1, moment2=moment2, weights=weights)


def reference(grads, basis, moment1, moment2, weights):
    total = jnp.float32(0.0)
    for index in range(MATS):
        grad_block = grads[index].astype(jnp.float32)
        total = total + jnp.sum(grad_block * grad_block)
    limit = 1.0 * math.sqrt(MATS * D * FF)
    scale = limit / jnp.maximum(jnp.sqrt(total), limit)
    first_bias_correction = 1.0 - 0.9 ** STEP
    second_fix = 1.0 - 0.999 ** STEP
    out_weights = []
    out_first = []
    out_second = []
    for index in range(MATS):
        base = basis[index].astype(jnp.float32)
        projected = jnp.dot(base.T, grads[index].astype(jnp.float32), preferred_element_type=jnp.float32)
        scaled = scale * projected
        first = 0.9 * moment1[index] + 0.1 * scaled
        second = 0.999 * moment2[index] + 0.001 * scaled * scaled
        low_rank_update = (first / first_bias_correction / (jnp.sqrt(second / second_fix) + 1e-08)).astype(jnp.bfloat16)
        projected_back = jnp.dot(base, low_rank_update.astype(jnp.float32), preferred_element_type=jnp.float32)
        out_weights.append((weights[index].astype(jnp.float32) - 0.5 * projected_back).astype(jnp.bfloat16))
        out_first.append(first)
        out_second.append(second)
    return (jnp.stack(out_weights), jnp.stack(out_first), jnp.stack(out_second))
```

```python
import math

import jax
import jax.numpy as jnp
from jax import lax
from jax.experimental import pallas as pl
from jax.experimental.pallas import tpu as pltpu
from jax.sharding import PartitionSpec as P

STEP = 10
SPLITS = 2


def moment_step(projected, moment1, moment2, scale):
    scaled = scale * projected
    first = 0.9 * moment1 + 0.1 * scaled
    second = 0.999 * moment2 + 0.001 * scaled * scaled
    first_bias_correction = 1.0 - 0.9**STEP
    second_fix = 1.0 - 0.999**STEP
    low_rank_update = (
        first / first_bias_correction / (jnp.sqrt(second / second_fix) + 1e-08)
    ).astype(jnp.bfloat16)
    return (first, second, low_rank_update)


def tile_of(width):
    tile = 128
    for cand in range(128, 1025, 128):
        if width % cand == 0:
            tile = cand
    return tile


def place(groups, pieces, out, shape, mat, split):
    count = len(pieces)
    rows, width = pieces[0].shape
    tile = tile_of(width)
    tiles = width // tile

    def piece_spec(p):
        def index(i, j, groups_ref):
            return (0, jnp.where(i == p, j, jnp.where(i < p, 0, tiles - 1)))

        return pl.BlockSpec((rows, tile), index)

    def out_index(i, j, groups_ref):
        return (mat, 0, groups_ref[i] * (SPLITS * tiles) + split * tiles + j)

    def kernel(groups_ref, *refs):
        out_ref = refs[-1]
        for p in range(count):

            @pl.when(pl.program_id(0) == p)
            def _():
                out_ref[0] = refs[p][...]

    extra = [] if out is None else [out]
    return pl.pallas_call(
        kernel,
        grid_spec=pltpu.PrefetchScalarGridSpec(
            num_scalar_prefetch=1,
            grid=(count, tiles),
            in_specs=[piece_spec(p) for p in range(count)]
            + [pl.BlockSpec(memory_space=pl.ANY) for _ in extra],
            out_specs=pl.BlockSpec((1, rows, tile), out_index),
        ),
        out_shape=jax.ShapeDtypeStruct(shape, pieces[0].dtype),
        input_output_aliases={} if out is None else {1 + count: 0},
        cost_estimate=pl.CostEstimate(
            flops=0, bytes_accessed=4 * count * rows * width, transcendentals=0
        ),
        name="place",
    )(groups, *pieces, *extra)


def solution(mesh):
    dp = mesh.shape["dp"]
    cores = 2 if dp % 2 == 0 else 1
    chips = dp // cores
    n = mesh.shape["rows"]
    ring = [2 * q if q < n // 2 else 2 * (n - 1 - q) + 1 for q in range(n)]

    def sum_all(x):
        if dp & (dp - 1) or n & (n - 1):
            return lax.psum(x, ("dp", "rows"))
        x = jnp.full((8, 128), x, jnp.float32)
        for axis, size in (("rows", n), ("dp", dp)):
            bit = 1
            while bit < size:
                x = x + lax.ppermute(x, axis, [(i, i ^ bit) for i in range(size)])
                bit *= 2
        return x[0, 0]

    def local(grads, basis, moment1, moment2, weights):
        mats, rows, cols = grads.shape
        width = cols // SPLITS
        limit = 1.0 * math.sqrt(mats * rows * mesh.shape["rows"] * cols * dp)

        chunks = [(m, s) for m in range(mats) for s in range(SPLITS)]

        def part(x, m, s):
            return x[m, :, s * width : (s + 1) * width]

        partials = [
            lax.dot_general(
                basis[m],
                part(grads, m, s),
                (((0,), (0,)), ((), ())),
                preferred_element_type=jnp.float32,
            )
            for m, s in chunks
        ]
        wide = grads.astype(jnp.float32)
        total = sum_all(jnp.sum(wide * wide))
        scale = limit / jnp.maximum(jnp.sqrt(total), limit)

        me = lax.axis_index("dp")
        chip, core = me // cores, me % cores
        order = [(k, c) for c in range(cores) for k in range(chips)]
        groups = jnp.stack(
            [((chip + chips - k) % chips) * cores + (core + c) % cores for k, c in order]
        ).astype(jnp.int32)

        def from_chip(x, k):
            pairs = [
                (a * cores + c, ((a + k) % chips) * cores + c)
                for a in range(chips)
                for c in range(cores)
            ]
            return lax.ppermute(x, "dp", pairs)

        def from_core(x):
            pairs = [
                (a * cores + c, a * cores + (c + 1) % cores)
                for a in range(chips)
                for c in range(cores)
            ]
            return lax.ppermute(x, "dp", pairs)

        tie = lax.optimization_barrier
        row = lax.axis_index("rows")
        pos = jnp.where(row % 2 == 0, row // 2, n - 1 - row // 2)
        height = moment1.shape[1]

        def start_of(q):
            q = (q + 2 * n) % n
            return jnp.where(q < n // 2, 2 * q, 2 * (n - 1 - q) + 1) * height

        def hop(x, way):
            return lax.ppermute(
                x, "rows", [(ring[q], ring[(q + way) % n]) for q in range(n)]
            )

        def block(partial, q):
            return lax.dynamic_slice_in_dim(partial, start_of(q), height, 0)

        def hops_of(i):
            near, far = (n - 1) // 2, n // 2
            return ((1, far), (-1, near)) if i % 2 == 0 else ((1, near), (-1, far))

        def reduce_pair(held):
            sums = [block(p, pos) for p in held]
            live = {}
            for i, p in enumerate(held):
                for way, far in hops_of(i):
                    if far:
                        live[i, way] = block(p, pos + way * far)
            for step in range(n // 2):
                for i, p in enumerate(held):
                    for way, far in hops_of(i):
                        if step >= far:
                            continue
                        got = hop(live[i, way], way)
                        if step == far - 1:
                            sums[i] = sums[i] + got
                        else:
                            live[i, way] = got + block(p, pos + way * (far - 1 - step))
            return sums

        def gather_pair(held):
            full = []
            for x in held:
                empty = jnp.zeros((height * n, x.shape[1]), x.dtype)
                full.append(lax.dynamic_update_slice_in_dim(empty, x, row * height, 0))
            live = {(i, way): x for i, x in enumerate(held) for way in (1, -1)}
            for step in range(n // 2):
                for i in range(len(held)):
                    for way, far in hops_of(i):
                        if step >= far:
                            continue
                        live[i, way] = hop(live[i, way], way)
                        full[i] = lax.dynamic_update_slice_in_dim(
                            full[i], live[i, way], start_of(pos - way * (step + 1)), 0
                        )
            return full

        firsts, seconds, exchanged = [], [], []

        def finish(number, pair, sums):
            updates = []
            for (m, s), projected in zip(pair, sums):
                first, second, update = moment_step(
                    projected, part(moment1, m, s), part(moment2, m, s), scale
                )
                firsts.append(first)
                seconds.append(second)
                updates.append(update)
            for (m, s), full in zip(pair, gather_pair(updates)):
                back = jnp.dot(basis[m], full, preferred_element_type=jnp.float32)
                fresh = part(weights, m, s).astype(jnp.float32) - 0.5 * back
                fresh = fresh.astype(jnp.bfloat16)
                exchanged.append([fresh] + [from_chip(fresh, k) for k in range(1, chips)])

        sums = None
        pairs = [chunks[i : i + 2] for i in range(0, len(chunks), 2)]
        for number, pair in enumerate(pairs):
            held = partials[2 * number : 2 * number + 2]
            if sums is not None:
                held, sums = tie((held, sums))
            sums_before, sums = sums, reduce_pair(held)
            if number >= 1:
                finish(number - 1, pairs[number - 1], sums_before)
                sums, exchanged[-2][1:] = tie((sums, exchanged[-2][1:]))
                sums, exchanged[-1][0] = tie((sums, exchanged[-1][0]))
        finish(len(pairs) - 1, pairs[-1], sums)

        shape = (mats, rows, cols * dp)
        out = None
        for i, (m, s) in enumerate(chunks):
            pieces = list(exchanged[i])
            if i == 2:
                pieces[1:], out = tie((pieces[1:], out))
            if cores == 2:
                pieces = pieces + [from_core(x) for x in pieces]
            out = place(groups, pieces, out, shape, m, s)

        def whole(parts):
            return jnp.stack(
                [
                    jnp.concatenate(parts[m * SPLITS : (m + 1) * SPLITS], axis=1)
                    for m in range(mats)
                ]
            )

        return (out, whole(firsts), whole(seconds))

    return jax.shard_map(
        local,
        mesh=mesh,
        in_specs=(
            P(None, "rows", "dp"),
            P(None, "rows", None),
            P(None, "rows", "dp"),
            P(None, "rows", "dp"),
            P(None, "rows", "dp"),
        ),
        out_specs=(P(None, "rows", None), P(None, "rows", "dp"), P(None, "rows", "dp")),
        check_vma=False,
    )
```
